8 devices in a mesh: dp: 2 (over z, y), tp: 4 (over x, core).
Axes of the slice: x: 2, y: 2, z: 1, core: 2. Of those that a mesh axis runs over, the one named last changes fastest.
Arguments:
- hidden: bfloat16 [32, 3, 3072], P('dp'), parts along dimension 0
- draft_ids: int32 [32, 2], P('dp'), parts along dimension 0
- norm_gain: bfloat16 [3072], replicated
- head_w: bfloat16 [3072, 128256], P(None, 'tp')
Outputs:
- output 1: float32 [32, 2], P('dp'), parts along dimension 0
- output 2: float32 [32, 3], P('dp'), parts along dimension 0
- output 3: float32 [32, 3], P('dp'), parts along dimension 0
There are 2 independent parts. The reference program is written for one: setup_inputs(seed, part) draws one part's arguments, and reference() takes and returns one part's arrays. A program takes and returns all parts, laid end to end along the dimension named above; an argument that names none is the same for every part.
All inputs are finite; a program needn't handle non-finite values.
Results may differ from the reference program's by a relative error of at most 0.001.
Values sent between devices are 32-bit elements.
A program may use at most 1 GiB of HBM per device.

```python
import jax
import jax.numpy as jnp
from jax import lax

DIM = 3072
VOCAB = 128256
BATCH = 16
DRAFTS = 2
NORM_EPS = 1e-5


def setup_inputs(seed: int = 0, part: int = 0) -> dict:
    root_key = jax.random.key(seed)
    shared_key, part_base = jax.random.split(root_key)
    part_key = jax.random.fold_in(part_base, part)
    key_x, key_d = jax.random.split(part_key)
    key_g, key_w, key_hot = jax.random.split(shared_key, 3)
    hidden = jax.random.normal(key_x, (BATCH, DRAFTS + 1, DIM), jnp.float32)
    draft_ids = jax.random.randint(key_d, (BATCH, DRAFTS), 0, VOCAB, jnp.int32)
    norm_gain = 1.0 + 0.2 * jax.random.normal(key_g, (DIM,), jnp.float32)
    hot_cols = jax.random.randint(key_hot, (VOCAB,), 0, 64, jnp.int32) == 0
    col_scale = jnp.where(hot_cols, 3.5, 2.0) * DIM ** -0.5
    head_w = jax.random.normal(key_w, (DIM, VOCAB), jnp.float32) * col_scale
    return {'hidden': hidden.astype(jnp.bfloat16), 'draft_ids': draft_ids, 'norm_gain': norm_gain.astype(jnp.bfloat16), 'head_w': head_w.astype(jnp.bfloat16)}


def rms_norm(hidden, norm_gain):
    wide_x = hidden.astype(jnp.float32)
    inv_rms = lax.rsqrt(jnp.mean(wide_x * wide_x, axis=-1, keepdims=True) + NORM_EPS)
    return (wide_x * inv_rms * norm_gain.astype(jnp.float32)).astype(jnp.bfloat16)


def reference(hidden, draft_ids, norm_gain, head_w):
    def one_sequence(seq_pair):
        seq_rows, seq_ids = seq_pair
        normed = rms_norm(seq_rows, norm_gain)
        logits = jnp.dot(normed, head_w, preferred_element_type=jnp.float32)
        row_max = jnp.max(logits, axis=-1)
        shifted = logits - row_max[:, None]
        exp_vals = jnp.exp(shifted)
        exp_sum = jnp.sum(exp_vals, axis=-1)
        weighted = jnp.sum(exp_vals * shifted, axis=-1)
        log_sum = jnp.log(exp_sum)
        log_norm = row_max + log_sum
        entropy = log_sum - weighted / exp_sum
        drafts = seq_ids.shape[0]
        picked = jnp.take_along_axis(logits[:drafts], seq_ids[:, None], axis=1)[:, 0]
        return picked - log_norm[:drafts], log_norm, entropy
    draft_logp, log_norm, entropy = lax.map(one_sequence, (hidden, draft_ids))
    return draft_logp, log_norm, entropy
```

```python
import functools

import jax
import jax.numpy as jnp
from jax import lax
from jax.experimental import pallas as pl
from jax.experimental.pallas import tpu as pltpu
from jax.sharding import PartitionSpec as P

NORM_EPS = 1e-5
DP, TP = 2, 4
LANES = 128
BLOCK = 1024
TAIL = 336
SLOTS = 8
PARTS = 4
MESH = pl.DeviceIdType.MESH
F32 = jnp.float32
LOWEST = float(jnp.finfo(jnp.float32).min)


def fold(m, s, w, m_new):
    d = jnp.maximum(m - m_new, LOWEST)
    a = jnp.exp(d)
    return a * s, a * (w + s * d)


def kernel(cfg, x_hbm, ids_hbm, gain_hbm, w_hbm, logp_ref, norm_ref, ent_ref,
           x_v, gain_v, ids_s, wbuf, nsend, nrecv, n_all, n_t, id_send, id_recv, stat, gath,
           x_sem, gain_sem, ids_sem, w_sem, ns_sem, nr_sem, rs_sem, rr_sem, id_sem, st_send, st_recv):
    seqs, toks, dim, cols, half, full, tails = cfg
    rows = seqs * toks
    part = dim // PARTS
    dp, tp = lax.axis_index("dp"), lax.axis_index("tp")
    core = lax.rem(tp, 2)
    base = dp * half

    x_copy = pltpu.make_async_copy(x_hbm, x_v, x_sem)
    gain_copy = pltpu.make_async_copy(gain_hbm, gain_v, gain_sem)
    ids_copy = pltpu.make_async_copy(ids_hbm, ids_s, ids_sem)
    x_copy.start()
    gain_copy.start()
    ids_copy.start()

    def block_copy(j, slot):
        start = pl.multiple_of(base + j * BLOCK, 32)
        return pltpu.make_async_copy(w_hbm.at[pl.ds(start, BLOCK), :], wbuf.at[slot], w_sem.at[slot])

    tail_slot = full % SLOTS

    def tail_copy(i):
        start = pl.multiple_of(base + full * BLOCK + i * TAIL, 16)
        return pltpu.make_async_copy(w_hbm.at[pl.ds(start, TAIL), :],
                                     wbuf.at[tail_slot, pl.ds(i * TAIL, TAIL), :], w_sem.at[SLOTS + i])

    for j in range(SLOTS):
        block_copy(j, j).start()

    barrier = pltpu.get_barrier_semaphore()
    others = [(a, b) for a in range(DP) for b in range(TP) if (a, b) != (0, 0)]

    def device(a, b):
        return (lax.rem(dp + a, DP), lax.rem(tp + b, TP))

    for a, b in others:
        pl.semaphore_signal(barrier, inc=1, device_id=device(a, b), device_id_type=MESH)

    x_copy.wait()
    gain_copy.wait()
    gain = gain_v[...].astype(F32)
    for t in range(toks):
        x = x_v[t].astype(F32)
        inv = lax.rsqrt(jnp.mean(x * x, axis=-1, keepdims=True) + NORM_EPS)
        n = (x * inv * gain).astype(jnp.bfloat16)
        n_all[pl.ds(t * seqs, seqs), :] = n
        for q in range(PARTS):
            nsend[q, pl.ds(t * seqs, seqs), :] = n[:, q * part:(q + 1) * part].astype(F32)
    n_all[pl.ds(2 * rows, LANES - 2 * rows), :] = jnp.zeros((LANES - 2 * rows, dim), jnp.bfloat16)
    ids_copy.wait()
    lane = lax.broadcasted_iota(jnp.int32, (8, LANES), 1)
    own_ids = jnp.full((8, LANES), -1, jnp.int32)
    for t in range(toks - 1):
        for b in range(seqs):
            own_ids = jnp.where(lane == t * seqs + b, ids_s[t, b], own_ids)
    id_send[...] = own_ids

    pl.semaphore_wait(barrier, len(others))

    mine = PARTS // 2
    sends = []
    for q in range(mine):
        p = core * mine + q
        sends.append(pltpu.make_async_remote_copy(
            nsend.at[p], nrecv.at[p], ns_sem.at[q], nr_sem.at[q], device_id=device(1, 0), device_id_type=MESH))
        sends[-1].start()
    id_copy = pltpu.make_async_remote_copy(
        id_send, id_recv, id_sem.at[0], id_sem.at[1], device_id=device(1, 0), device_id_type=MESH)
    id_copy.start()
    partner = (dp, tp + 1 - 2 * core)
    relays = []
    for q in range(mine):
        sends[q].wait_recv()
        p = core * mine + q
        relays.append(pltpu.make_async_remote_copy(
            nrecv.at[p], nrecv.at[p], rs_sem.at[q], rr_sem.at[q], device_id=partner, device_id_type=MESH))
        relays[-1].start()
    id_copy.wait_recv()
    ids = jnp.where((lane >= rows) & (lane < 2 * rows), pltpu.roll(id_recv[...], rows, 1), own_ids)
    for q in range(mine):
        relays[q].wait_recv()
    for q in range(PARTS):
        n_all[pl.ds(rows, rows), pl.ds(q * part, part)] = nrecv[q].astype(jnp.bfloat16)
    n_t[...] = n_all[...].T

    first = tp * cols + base
    offset = ids - first - lax.broadcasted_iota(jnp.int32, (8, LANES), 0)

    def update(carry, w_block, size, begin):
        m, s, w, picked = carry
        z = jnp.dot(w_block, n_t[...], preferred_element_type=F32).reshape(size // 8, 8, LANES)
        m_new = jnp.maximum(m, jnp.max(z, axis=0))
        s, w = fold(m, s, w, m_new)
        shifted = z - m_new[None]
        e = jnp.exp(shifted)
        s = s + jnp.sum(e, axis=0)
        w = w + jnp.sum(e * shifted, axis=0)
        at = 8 * lax.broadcasted_iota(jnp.int32, (size // 8, 8, LANES), 0)
        picked = picked + jnp.sum(jnp.where((offset - begin)[None] == at, z, 0.0), axis=0)
        return m_new, s, w, picked

    def step(j, carry):
        slot = lax.rem(j, SLOTS)
        block_copy(j, slot).wait()
        carry = update(carry, wbuf[slot], BLOCK, j * BLOCK)

        @pl.when(j + SLOTS < full)
        def _():
            block_copy(j + SLOTS, slot).start()

        @pl.when(j + SLOTS == full)
        def _():
            for i in range(tails):
                tail_copy(i).start()

        return carry

    zero = jnp.zeros((8, LANES), F32)
    carry = lax.fori_loop(0, full, step, (jnp.full((8, LANES), LOWEST, F32), zero, zero, zero))
    for i in range(tails):
        tail_copy(i).wait()
        carry = update(carry, wbuf[tail_slot, pl.ds(i * TAIL, TAIL), :], TAIL, full * BLOCK + i * TAIL)
    m, s, w, picked = carry

    top = jnp.max(m, axis=0, keepdims=True)
    s, w = fold(m, s, w, top)
    stat[0:1, :] = top
    stat[1:2, :] = jnp.sum(s, axis=0, keepdims=True)
    stat[2:3, :] = jnp.sum(w, axis=0, keepdims=True)
    stat[3:4, :] = jnp.sum(picked, axis=0, keepdims=True)
    stat[4:8, :] = jnp.zeros((4, LANES), F32)
    stat_copies = []
    for i, (a, b) in enumerate(others):
        stat_copies.append(pltpu.make_async_remote_copy(
            stat, gath.at[i], st_send.at[i], st_recv.at[i], device_id=device(a, b), device_id_type=MESH))
        stat_copies[-1].start()
    tiles = [stat[...]]
    for i, (a, b) in enumerate(others):
        stat_copies[i].wait_recv()
        tile = gath[i]
        tiles.append(tile if a == 0 else pltpu.roll(tile, LANES - rows, 1))
    top = functools.reduce(jnp.maximum, [t[0:1, :] for t in tiles])
    parts = [fold(t[0:1, :], t[1:2, :], t[2:3, :], top) for t in tiles]
    s = sum(q[0] for q in parts)
    w = sum(q[1] for q in parts)
    picked = sum(t[3:4, :] for t in tiles)
    log_s = jnp.log(s)
    log_norm = top + log_s
    entropy = log_s - w / s
    logp = picked - log_norm
    for t in range(toks):
        shift = (LANES - t * seqs) % LANES
        norm_ref[t:t + 1, :] = pltpu.roll(log_norm, shift, 1)[:, :seqs]
        ent_ref[t:t + 1, :] = pltpu.roll(entropy, shift, 1)[:, :seqs]
        if t < toks - 1:
            logp_ref[t:t + 1, :] = pltpu.roll(logp, shift, 1)[:, :seqs]

    for copy in sends + relays + [id_copy] + stat_copies:
        copy.wait_send()


def solution(mesh):
    def per_device(hidden, draft_ids, norm_gain, head_w):
        seqs, toks, dim = hidden.shape
        cols = head_w.shape[1]
        half = cols // DP
        full = half // BLOCK
        tails = (half - full * BLOCK) // TAIL
        assert half == full * BLOCK + tails * TAIL
        rows = seqs * toks
        cfg = (seqs, toks, dim, cols, half, full, tails)
        any_spec = pl.BlockSpec(memory_space=pl.ANY)
        vmem_spec = pl.BlockSpec(memory_space=pltpu.VMEM)
        dma = pltpu.SemaphoreType.DMA
        mine = PARTS // 2
        logp, norm, ent = pl.pallas_call(
            functools.partial(kernel, cfg),
            out_shape=[jax.ShapeDtypeStruct((toks - 1, seqs), F32),
                       jax.ShapeDtypeStruct((toks, seqs), F32),
                       jax.ShapeDtypeStruct((toks, seqs), F32)],
            in_specs=[any_spec] * 4,
            out_specs=[vmem_spec] * 3,
            scratch_shapes=[
                pltpu.VMEM((toks, seqs, dim), jnp.bfloat16),
                pltpu.VMEM((1, dim), jnp.bfloat16),
                pltpu.SMEM((toks - 1, seqs), jnp.int32),
                pltpu.VMEM((SLOTS, BLOCK, dim), jnp.bfloat16),
                pltpu.VMEM((PARTS, rows, dim // PARTS), F32),
                pltpu.VMEM((PARTS, rows, dim // PARTS), F32),
                pltpu.VMEM((LANES, dim), jnp.bfloat16),
                pltpu.VMEM((dim, LANES), jnp.bfloat16),
                pltpu.VMEM((8, LANES), jnp.int32),
                pltpu.VMEM((8, LANES), jnp.int32),
                pltpu.VMEM((8, LANES), F32),
                pltpu.VMEM((DP * TP - 1, 8, LANES), F32),
                dma, dma, dma, dma((SLOTS + 2,)), dma((mine,)), dma((mine,)), dma((mine,)), dma((mine,)),
                dma((2,)), dma((DP * TP - 1,)), dma((DP * TP - 1,)),
            ],
            compiler_params=pltpu.CompilerParams(
                collective_id=0, has_side_effects=True, vmem_limit_bytes=66_000_000),
        )(hidden.transpose(1, 0, 2), draft_ids.T, norm_gain.reshape(1, dim), head_w.T)
        return logp.T, norm.T, ent.T

    specs_in = (P('dp', None, None), P('dp', None), P(None), P(None, 'tp'))
    specs_out = (P('dp', None), P('dp', None), P('dp', None))
    return jax.shard_map(per_device, mesh=mesh, in_specs=specs_in, out_specs=specs_out, check_vma=False)
```
